512 devices in a mesh: seq: 8 (over x, core), dp: 8 (over z), tensor: 8 (over y).
Axes of the slice: x: 4, y: 8, z: 8, core: 2. Of those that a mesh axis runs over, the one named last changes fastest.
Arguments:
- queries: bfloat16 [8, 3072, 2048], P('dp', ('seq', 'tensor')), may hold values from -128 to 128
- key_vectors: bfloat16 [8, 3072, 2048], P('dp', ('seq', 'tensor')), may hold values from -6 to 6
- values: bfloat16 [8, 3072, 2048], P('dp', ('seq', 'tensor')), may hold values from -6 to 6
- out_grad: bfloat16 [8, 3072, 2048], P('dp', ('seq', 'tensor')), may hold values from -6 to 6
- positions: int32 [8, 3072], P('dp', 'seq'), may hold values from -1 to 16383, as said below
- sink_logits: float32 [16], P('tensor'), may hold values from -1 to 3
Outputs:
- attended: bfloat16 [8, 3072, 2048], P('dp', ('seq', 'tensor'))
- query_grad: bfloat16 [8, 3072, 2048], P('dp', ('seq', 'tensor'))
- key_grad: bfloat16 [8, 3072, 2048], P('dp', ('seq', 'tensor'))
- value_grad: bfloat16 [8, 3072, 2048], P('dp', ('seq', 'tensor'))
- sink_grad: float32 [16], P('tensor')
The draws below stay inside these ranges and needn't reach their ends.
Inputs may be any that keep to these rules, and one draw needn't show every extreme that they name: Each document's tokens 0 to 16383 form slabs of 4096 tokens; each slab keeps exactly 512 routed tokens, its first half on one sequence shard of 384 slots and its second half on the next. A shard lists its routed positions in rising order in its first slots and -1 in the slots left over; it holds 128 to 384 routed tokens, and some shard of every document holds 384.
All inputs are finite; a program needn't handle non-finite values.
Results may differ from the reference program's by a relative error of at most 0.02.
Values may be sent and summed in bfloat16 or wider, within the bound.
A program may use at most 64 MiB of HBM per device.

```python
import jax
import jax.numpy as jnp
from jax import lax

SLAB = 4096
HEADS = 16
DH = 128
KEEP = 512
CAP = 384
DOCS = 8
SLOTS = 3072


def query_key_pair(key):
    base_key = jax.random.fold_in(key, 7)
    query_key, key_key = jax.random.split(base_key)
    shape = (DOCS, SLOTS, HEADS * DH)
    query_draw = jnp.clip(jax.random.normal(query_key, shape, jnp.float32), -6.0, 6.0)
    key_draw = jnp.clip(jax.random.normal(key_key, shape, jnp.float32), -6.0, 6.0)
    return (query_draw.astype(jnp.bfloat16), key_draw.astype(jnp.bfloat16))


def draw_queries(key, part):
    return query_key_pair(key)[0]


def draw_key_vectors(key, part):
    return query_key_pair(key)[1]


def draw_positions(key, part):
    base_key = jax.random.fold_in(key, 11)
    count_key, forced_key, choice_key = jax.random.split(base_key, 3)
    half_slab = SLAB // 2
    slab_count = SLOTS // (2 * CAP)
    counts = jax.random.randint(count_key, (DOCS, slab_count), KEEP - CAP, CAP + 1)
    forced = jax.random.randint(forced_key, (DOCS,), 0, slab_count)
    counts = jnp.where(jnp.arange(slab_count)[None, :] == forced[:, None], CAP, counts)
    shard_counts = jnp.stack([counts, KEEP - counts], axis=2).reshape(DOCS * 2 * slab_count)
    shard_keys = jax.random.split(choice_key, DOCS * 2 * slab_count)
    shard_ids = jnp.tile(jnp.arange(2 * slab_count, dtype=jnp.int32), DOCS)

    def one_shard(sub_key, count, shard_id):
        shuffled = jax.random.permutation(sub_key, half_slab)
        ranking = jnp.argsort(shuffled, stable=True)
        chosen = ranking < count
        slot_index = jnp.cumsum(chosen.astype(jnp.int32)) - 1
        slot_index = jnp.where(chosen, slot_index, CAP)
        token_place = jnp.arange(half_slab, dtype=jnp.int32) + shard_id * half_slab
        return jnp.full((CAP,), -1, jnp.int32).at[slot_index].set(token_place, mode='drop')
    lists = jax.vmap(one_shard)(shard_keys, shard_counts, shard_ids)
    return lists.reshape(DOCS, SLOTS)


def shard_levels(own_key, shape, cuts, smallest, largest):
    level, own = 1.0, jax.random.fold_in(own_key, 6)
    for axis_at, blocks in cuts:
        steps = jnp.exp(jax.random.uniform(jax.random.fold_in(own, axis_at), (blocks,), jnp.float32, smallest / len(cuts), largest / len(cuts)))
        level = level * jnp.repeat(steps, shape[axis_at] // blocks).reshape([-1 if axis == axis_at else 1 for axis in range(len(shape))])
    return level


def centred(rng, shape, scale, reach, cuts=(), held_as=jnp.bfloat16):
    entries = jax.random.normal(rng, shape, jnp.float32) * scale
    if len(cuts) > 0:
        entries = shard_levels(rng, shape, cuts, -0.22, 0.18) * entries
    return jnp.clip(entries, min=-reach, max=reach).astype(held_as)


def setup_inputs(seed: int = 0) -> dict:
    splits = jax.random.split(jax.random.key(seed), 7)
    queries = draw_queries(jax.random.fold_in(splits[6], 71), 0)
    key_vectors = draw_key_vectors(jax.random.fold_in(splits[6], 71), 0)
    values = centred(splits[2], (DOCS, SLOTS, HEADS * DH), 1.0, 6.0, ((0, 8), (1, 64)))
    out_grad = centred(splits[3], (DOCS, SLOTS, HEADS * DH), 1.0, 6.0, ((0, 8), (1, 64)))
    positions = draw_positions(jax.random.fold_in(splits[6], 71), 0)
    sink_logits = jnp.clip(-1.0 + 4.0 * jax.random.uniform(splits[5], (HEADS,), jnp.float32) ** shard_levels(splits[5], (HEADS,), ((0, 8),), -0.2, 0.2), -1.0, 3.0)
    return dict(queries=queries, key_vectors=key_vectors, values=values, out_grad=out_grad, positions=positions, sink_logits=sink_logits)


def head_pass(head_inputs, positions_doc):
    query_head, key_head, value_head, grad_head, sink = head_inputs
    raw_scores = jnp.dot(query_head, key_head.T, preferred_element_type=jnp.float32)
    scores = raw_scores * (DH ** -0.5)
    visible = (positions_doc[None, :] <= positions_doc[:, None]) & (positions_doc[None, :] >= 0)
    scores = jnp.where(visible, scores, -1e30)
    row_max = jnp.maximum(jnp.max(scores, axis=1), sink)
    row_total = jnp.exp(sink - row_max) + jnp.sum(jnp.exp(scores - row_max[:, None]), axis=1)
    weights_full = jnp.exp(scores - row_max[:, None]) / row_total[:, None]
    weights_half = weights_full.astype(jnp.bfloat16)
    attended = jnp.dot(weights_half, value_head, preferred_element_type=jnp.float32).astype(jnp.bfloat16)
    delta_rows = jnp.sum(attended.astype(jnp.float32) * grad_head.astype(jnp.float32), axis=1)
    value_dots = jnp.dot(grad_head, value_head.T, preferred_element_type=jnp.float32)
    score_grad = (weights_full * (value_dots - delta_rows[:, None]) * (DH ** -0.5)).astype(jnp.bfloat16)
    query_grad = jnp.dot(score_grad, key_head, preferred_element_type=jnp.float32).astype(jnp.bfloat16)
    key_grad = jnp.dot(score_grad.T, query_head, preferred_element_type=jnp.float32).astype(jnp.bfloat16)
    value_grad = jnp.dot(weights_half.T, grad_head, preferred_element_type=jnp.float32).astype(jnp.bfloat16)
    sink_term = -jnp.sum(jnp.exp(sink - row_max) / row_total * delta_rows)
    return attended, query_grad, key_grad, value_grad, sink_term


def reference(queries, key_vectors, values, out_grad, positions, sink_logits):
    slot_count = queries.shape[1]
    head_count = queries.shape[2] // DH

    def split_heads(matrix):
        return matrix.reshape(slot_count, head_count, DH).transpose(1, 0, 2)

    def join_heads(stacked):
        return stacked.transpose(1, 0, 2).reshape(slot_count, head_count * DH)

    def document_pass(doc_inputs):
        query_doc, key_doc, value_doc, grad_doc, positions_doc = doc_inputs

        def one_head(head_inputs):
            return head_pass(head_inputs, positions_doc)

        outs = lax.map(one_head, (split_heads(query_doc), split_heads(key_doc), split_heads(value_doc), split_heads(grad_doc), sink_logits))
        return join_heads(outs[0]), join_heads(outs[1]), join_heads(outs[2]), join_heads(outs[3]), outs[4]

    attended, query_grad, key_grad, value_grad, sink_terms = lax.map(document_pass, (queries, key_vectors, values, out_grad, positions))
    return attended, query_grad, key_grad, value_grad, jnp.sum(sink_terms, axis=0)
```

```python
import functools

import jax
import jax.numpy as jnp
from jax import lax
from jax.experimental import pallas as pl
from jax.experimental.pallas import tpu as pltpu
from jax.sharding import PartitionSpec as P

DH = 128
CHIPS = 4
CORES = 2
LOG2E = 1.4426950408889634
NEG = -1e30
MESH = pl.DeviceIdType.MESH
BF = jnp.bfloat16
F32 = jnp.float32

DIRECT = (
    (0, 1, 0, 0),
    (0, 3, 0, 1),
    (0, 1, 0, 1),
    (0, 3, 0, 0),
    (1, 2, 1, 0),
    (1, 0, 1, 1),
    (1, 2, 1, 1),
    (2, 3, 2, 0),
    (2, 3, 2, 1),
)
RELAY = ((1, 2, 0, 0), (3, 2, 0, 1), (2, 3, 1, 0), (0, 3, 1, 1))
FIRST = (
    (3, 0, 1, 1, 0),
    (3, 2, 1, 0, 0),
    (3, 0, 0, 0, 2),
    (3, 2, 2, 0, 1),
    (3, 2, 2, 1, 2),
    (2, 1, 0, 0, 0),
    (2, 3, 0, 1, 0),
    (2, 1, 1, 1, 2),
    (1, 0, 0, 1, 3),
)
SECOND = ((3, 0, 0, 1, 4), (2, 1, 1, 0, 1), (1, 0, 0, 0, 1), (0, 1, 1, 1, 3))
FINAL = {
    0: ((0, (1, 2)), (1, (3, 4))),
    1: ((0, (1,)), (1, (2, 3))),
    2: ((0, (1,)), (1, (2,))),
    3: (),
}


def contract(a, b, dims):
    return lax.dot_general(a, b, ((dims[:1], dims[1:]), ((), ())), preferred_element_type=F32)


def kernel(
    tensor_count,
    dp_count,
    q_hbm,
    k_hbm,
    v_hbm,
    g_hbm,
    pos_ref,
    sink_ref,
    att_out,
    dq_out,
    dk_out,
    dv_out,
    sink_out,
    q_s,
    g_s,
    k_s,
    v_s,
    scores,
    probs,
    sgrad,
    pos_src,
    pos_all,
    pos_col,
    att_t,
    dq_t,
    att_s,
    dq_s,
    dk_f,
    dv_f,
    dk_b,
    dv_b,
    dk_r,
    dv_r,
    sink_src,
    sink_seq,
    sink_mid,
    sink_dp,
    in_send,
    in_recv,
    pos_send,
    pos_recv,
    gx_send,
    gx_recv,
    rx_send,
    rx_recv,
    out_send,
    out_recv,
    sink_send,
    sink_recv,
):
    seq = lax.axis_index("seq")
    dp = lax.axis_index("dp")
    t = lax.axis_index("tensor")
    x = lax.div(seq, CORES)
    c = lax.rem(seq, CORES)
    rows = q_hbm.shape[1]
    cap = rows * tensor_count
    slab = CORES * cap
    seq_count = CHIPS * CORES
    part = slab // 3

    peers = [(dc, dt) for dt in range(tensor_count) for dc in range(CORES)][1:]
    order = []
    for step in range(1, tensor_count // 2 + 1):
        for dt in (step, tensor_count - step):
            for dc in range(CORES):
                if (dc, dt) in peers and (dc, dt) not in order:
                    order.append((dc, dt))
    order = order + [p for p in peers if p not in order]

    def peer(dc, dt):
        return lax.rem(c + dc, CORES), lax.rem(t + dt, tensor_count)

    def seq_peer(d):
        return lax.rem(seq + d, seq_count)

    barrier = pltpu.get_barrier_semaphore()
    greeted = 0
    for dc, dt in order:
        if dt == 0:
            continue
        pc, pt = peer(dc, dt)
        pl.semaphore_signal(
            barrier, inc=1, device_id={"seq": x * CORES + pc, "tensor": pt}, device_id_type=MESH
        )
        greeted += 1
    for d in range(1, seq_count):
        pl.semaphore_signal(barrier, inc=1, device_id={"seq": seq_peer(d)}, device_id_type=MESH)
        greeted += 1
    for d in range(1, dp_count):
        pl.semaphore_signal(
            barrier, inc=1, device_id={"dp": lax.rem(dp + d, dp_count)}, device_id_type=MESH
        )
        greeted += 1

    pos_row = pos_ref[...]
    pos_src[...] = jnp.broadcast_to(pos_row, (8, cap))
    pos_all[seq] = jnp.broadcast_to(pos_row, (8, cap))
    pl.semaphore_wait(barrier, greeted)

    def remote(src, dst, send, recv, **where):
        return pltpu.make_async_remote_copy(
            src_ref=src, dst_ref=dst, send_sem=send, recv_sem=recv, device_id=where, device_id_type=MESH
        )

    def head_cols(pc, pt):
        return pl.ds(pl.multiple_of((pt * CORES + pc) * DH, DH), DH)

    def row_block(pc, pt):
        return pl.ds(pl.multiple_of(pc * cap + pt * rows, rows), rows)

    mine = row_block(c, t)

    def send_rows(n, src, dst):
        for dc, dt in order:
            pc, pt = peer(dc, dt)
            remote(
                src.at[0, :, head_cols(pc, pt)],
                dst.at[mine, :],
                in_send.at[n],
                in_recv.at[n],
                seq=x * CORES + pc,
                tensor=pt,
            ).start()
        pltpu.make_async_copy(
            src.at[0, :, head_cols(c, t)], dst.at[mine, :], in_recv.at[n]
        ).start()

    def pos_copy(d):
        return remote(
            pos_src, pos_all.at[seq], pos_send.at[d], pos_recv.at[d], seq=seq_peer(d)
        )

    send_rows(0, k_hbm, k_s.at[x])
    for d in range(1, seq_count):
        pos_copy(d).start()
    send_rows(1, v_hbm, v_s.at[x])
    send_rows(2, q_hbm, q_s)
    send_rows(3, g_hbm, g_s)

    def got_rows(n):
        pltpu.make_async_copy(q_s, q_s, in_recv.at[n]).wait()

    def half_rows(h):
        return pl.ds(h * cap, cap)

    def gather_copy(a, buf, n, move):
        _, to, j, h = move
        return remote(
            buf.at[j, half_rows(h), :],
            buf.at[j, half_rows(h), :],
            gx_send.at[a, n],
            gx_recv.at[a, j, h],
            seq=to * CORES + c,
        )

    def gather_wait(a, buf, j, h):
        ref = buf.at[j, half_rows(h), :]
        pltpu.make_async_copy(ref, ref, gx_recv.at[a, j, h]).wait()

    def gather_direct(a, buf):
        for i in range(CHIPS):

            @pl.when(x == i)
            def _():
                for n, move in enumerate(DIRECT):
                    if move[0] == i:
                        gather_copy(a, buf, n, move).start()

    def gather_relay(a, buf):
        for n, move in enumerate(RELAY):

            @pl.when(x == move[0])
            def _():
                gather_wait(a, buf, move[2], move[3])
                gather_copy(a, buf, len(DIRECT) + n, move).start()

    def gather_rest(a, buf):
        for i in range(CHIPS):
            relayed = [m[2:] for m in RELAY if m[0] == i]
            rest = [m[2:] for m in DIRECT + RELAY if m[1] == i and m[2:] not in relayed]
            if rest:

                @pl.when(x == i)
                def _():
                    for j, h in rest:
                        gather_wait(a, buf, j, h)

    got_rows(0)
    gather_direct(0, k_s)

    for d in range(1, seq_count):
        pltpu.make_async_copy(pos_src, pos_all.at[seq], pos_recv.at[d]).wait()

    def column(s, _):
        held = pos_all[s][:1, :]
        held = jnp.where(held < 0, jnp.int32(1 << 30), held)
        wide = jnp.broadcast_to(held, (DH, cap)).astype(F32)
        pos_col[pl.ds(pl.multiple_of(s * cap, cap), cap), :] = wide.T
        return 0

    lax.fori_loop(0, seq_count, column, 0)
    pos_q = jnp.concatenate(
        [pos_all[x * CORES][:1, :], pos_all[x * CORES + 1][:1, :]], axis=1
    ).astype(F32)

    got_rows(1)
    gather_direct(1, v_s)
    gather_relay(0, k_s)
    got_rows(2)

    sink2 = sink_ref[c] * LOG2E
    to_log2 = DH**-0.5 * LOG2E

    def score_block(b, carry):
        row_max, total = carry
        at = pl.ds(pl.multiple_of(b * part, part), part)
        j = lax.div(b, 3)
        inner = pl.ds(pl.multiple_of(lax.rem(b, 3) * part, part), part)
        s = contract(k_s[j, inner, :], q_s[...], (1, 1)) * to_log2
        pos_k = jnp.concatenate([pos_col[at, :]] * (slab // DH), axis=1)
        s = jnp.where(pos_k <= pos_q, s, NEG)
        scores[at, :] = s
        new_max = jnp.maximum(row_max, jnp.max(s, axis=0, keepdims=True))
        total = total * jnp.exp2(row_max - new_max) + jnp.sum(
            jnp.exp2(s - new_max), axis=0, keepdims=True
        )
        return new_max, total

    start = (jnp.full((1, slab), sink2, F32), jnp.ones((1, slab), F32))
    carry = lax.fori_loop(x * 3, x * 3 + 3, score_block, start)
    gather_relay(1, v_s)
    gather_rest(0, k_s)
    row_max, total = lax.fori_loop(0, x * 3, score_block, carry)
    lse = row_max + jnp.log2(total)

    gather_rest(1, v_s)
    att_t[...] = jnp.zeros_like(att_t)

    def attend_slab(j, _):
        def prob_block(i, _):
            at = pl.ds(pl.multiple_of(j * slab + i * part, part), part)
            probs[at, :] = jnp.exp2(scores[at, :] - lse).astype(BF)
            return 0

        lax.fori_loop(0, 3, prob_block, 0)
        whole = pl.ds(pl.multiple_of(j * slab, slab), slab)
        att_t[...] += contract(v_s[j], probs[whole, :], (0, 0))
        return 0

    lax.fori_loop(0, x + 1, attend_slab, 0)
    att_s[...] = att_t[...].T.astype(BF)

    def send_heads(n, src, dst):
        for dc, dt in order:
            pc, pt = peer(dc, dt)
            remote(
                src.at[row_block(pc, pt), :],
                dst.at[0, :, head_cols(c, t)],
                out_send.at[n],
                out_recv.at[n],
                seq=x * CORES + pc,
                tensor=pt,
            ).start()
        pltpu.make_async_copy(
            src.at[mine, :], dst.at[0, :, head_cols(c, t)], out_recv.at[n]
        ).start()

    send_heads(0, att_s, att_out)
    got_rows(3)

    delta = jnp.sum(
        att_s[...].astype(F32).T * g_s[...].astype(F32).T, axis=0, keepdims=True
    )

    own_sink = -jnp.sum(jnp.exp2(sink2 - lse) * delta)
    lane = lax.broadcasted_iota(jnp.int32, (8, DH), 1)
    own_tile = jnp.where(lane == c, own_sink, 0.0)
    sink_src[...] = own_tile
    sink_seq[seq] = own_tile

    def sink_seq_copy(d):
        return remote(
            sink_src, sink_seq.at[seq], sink_send.at[0, d], sink_recv.at[0, d], seq=seq_peer(d)
        )

    def sink_dp_copy(d):
        return remote(
            sink_mid,
            sink_dp.at[dp],
            sink_send.at[1, d],
            sink_recv.at[1, d],
            dp=lax.rem(dp + d, dp_count),
        )

    for d in range(1, seq_count):
        sink_seq_copy(d).start()

    def value_slab(j, _):
        whole = pl.ds(pl.multiple_of(j * slab, slab), slab)
        out = contract(probs[whole, :], g_s[...], (1, 0))
        dv_f[j] = out
        dv_b[j] = out.astype(BF)
        return 0

    lax.fori_loop(0, x + 1, value_slab, 0)

    def reduce_copy(a, buf, got, n, move):
        _, to, j, h, slot = move
        return remote(
            buf.at[j, half_rows(h), :],
            got.at[slot],
            rx_send.at[a, n],
            rx_recv.at[a, slot],
            seq=to * CORES + c,
        )

    def reduce_wait(a, got, slot):
        pltpu.make_async_copy(got.at[slot], got.at[slot], rx_recv.at[a, slot]).wait()

    def reduce_first(a, buf, got):
        for i in range(CHIPS):

            @pl.when(x == i)
            def _():
                for n, move in enumerate(FIRST):
                    if move[0] == i:
                        reduce_copy(a, buf, got, n, move).start()

    def reduce_second(a, own, buf, got):
        for n, move in enumerate(SECOND):
            i, to, j, h, slot = move

            @pl.when(x == i)
            def _():
                reduce_wait(a, got, 0)
                if i == 0:
                    buf[j, half_rows(h), :] = got[0]
                else:
                    buf[j, half_rows(h), :] = (
                        own[j, half_rows(h), :] + got[0].astype(F32)
                    ).astype(BF)
                reduce_copy(a, buf, got, len(FIRST) + n, move).start()

    def reduce_last(a, own, buf, got):
        for i in range(CHIPS):
            for h, slots in FINAL[i]:

                @pl.when(x == i)
                def _():
                    total = own[i, half_rows(h), :]
                    for slot in slots:
                        reduce_wait(a, got, slot)
                        total = total + got[slot].astype(F32)
                    buf[i, half_rows(h), :] = total.astype(BF)

    reduce_first(0, dv_b, dv_r)
    dq_t[...] = jnp.zeros_like(dq_t)

    def grad_slab(j, _):
        def grad_block(i, _):
            at = pl.ds(pl.multiple_of(j * slab + i * part, part), part)
            inner = pl.ds(pl.multiple_of(i * part, part), part)
            dots = contract(v_s[j, inner, :], g_s[...], (1, 1))
            sgrad[inner, :] = (jnp.exp2(scores[at, :] - lse) * (dots - delta)).astype(BF)
            return 0

        lax.fori_loop(0, 3, grad_block, 0)
        out = contract(sgrad[...], q_s[...], (1, 0)) * DH**-0.5
        dk_f[j] = out
        dk_b[j] = out.astype(BF)
        dq_t[...] += contract(k_s[j], sgrad[...], (0, 0))
        return 0

    lax.fori_loop(0, x + 1, grad_slab, 0)
    reduce_first(1, dk_b, dk_r)
    dq_s[...] = (dq_t[...] * DH**-0.5).T.astype(BF)
    send_heads(1, dq_s, dq_out)

    for d in range(1, seq_count):
        pltpu.make_async_copy(sink_src, sink_src, sink_recv.at[0, d]).wait()
    seq_sum = jnp.sum(sink_seq[...], axis=0)
    sink_mid[...] = seq_sum
    sink_dp[dp] = seq_sum
    for d in range(1, dp_count):
        sink_dp_copy(d).start()

    reduce_second(0, dv_f, dv_b, dv_r)
    reduce_last(0, dv_f, dv_b, dv_r)
    send_heads(3, dv_b.at[x], dv_out)
    reduce_second(1, dk_f, dk_b, dk_r)
    reduce_last(1, dk_f, dk_b, dk_r)
    send_heads(2, dk_b.at[x], dk_out)

    for d in range(1, dp_count):
        pltpu.make_async_copy(sink_mid, sink_mid, sink_recv.at[1, d]).wait()
    sink_out[...] = jnp.sum(sink_dp[...], axis=0)

    sent = q_s.at[pl.ds(0, slab - rows), :]
    for n in range(4):
        pltpu.make_async_copy(sent, sent, in_send.at[n]).wait()
        pltpu.make_async_copy(sent, sent, out_send.at[n]).wait()
        pltpu.make_async_copy(q_s, q_s, out_recv.at[n]).wait()
    for d in range(1, seq_count):
        pltpu.make_async_copy(pos_src, pos_src, pos_send.at[d]).wait()
        pltpu.make_async_copy(sink_src, sink_src, sink_send.at[0, d]).wait()
    for d in range(1, dp_count):
        pltpu.make_async_copy(sink_mid, sink_mid, sink_send.at[1, d]).wait()
    for i in range(CHIPS):

        @pl.when(x == i)
        def _():
            for a in range(2):
                half = k_s.at[0, half_rows(0), :]
                for n, move in enumerate(DIRECT + RELAY):
                    if move[0] == i:
                        pltpu.make_async_copy(half, half, gx_send.at[a, n]).wait()
                for n, move in enumerate(FIRST + SECOND):
                    if move[0] == i:
                        pltpu.make_async_copy(half, half, rx_send.at[a, n]).wait()


def on_device(queries, key_vectors, values, out_grad, positions, sink_logits):
    tensor_count = lax.axis_size("tensor")
    dp_count = lax.axis_size("dp")
    _, rows, features = queries.shape
    cap = rows * tensor_count
    slab = CORES * cap
    seq_count = CHIPS * CORES
    hbm = pl.BlockSpec(memory_space=pl.ANY)
    vmem = pl.BlockSpec(memory_space=pltpu.VMEM)
    smem = pl.BlockSpec(memory_space=pltpu.SMEM)
    row_type = jax.ShapeDtypeStruct((1, rows, features), BF)
    dma = pltpu.SemaphoreType.DMA
    moves = len(DIRECT) + len(RELAY)
    hops = len(FIRST) + len(SECOND)
    outs = pl.pallas_call(
        functools.partial(kernel, tensor_count, dp_count),
        out_shape=(row_type,) * 4 + (jax.ShapeDtypeStruct((8, DH), F32),),
        in_specs=[hbm] * 4 + [vmem, smem],
        out_specs=(hbm,) * 4 + (vmem,),
        scratch_shapes=[
            pltpu.VMEM((slab, DH), BF),
            pltpu.VMEM((slab, DH), BF),
            pltpu.VMEM((CHIPS, slab, DH), BF),
            pltpu.VMEM((CHIPS, slab, DH), BF),
            pltpu.VMEM((CHIPS * slab, slab), F32),
            pltpu.VMEM((CHIPS * slab, slab), BF),
            pltpu.VMEM((slab, slab), BF),
            pltpu.VMEM((8, cap), jnp.int32),
            pltpu.VMEM((seq_count, 8, cap), jnp.int32),
            pltpu.VMEM((seq_count * cap, DH), F32),
            pltpu.VMEM((DH, slab), F32),
            pltpu.VMEM((DH, slab), F32),
            pltpu.VMEM((slab, DH), BF),
            pltpu.VMEM((slab, DH), BF),
            pltpu.VMEM((CHIPS, slab, DH), F32),
            pltpu.VMEM((CHIPS, slab, DH), F32),
            pltpu.VMEM((CHIPS, slab, DH), BF),
            pltpu.VMEM((CHIPS, slab, DH), BF),
            pltpu.VMEM((5, cap, DH), BF),
            pltpu.VMEM((5, cap, DH), BF),
            pltpu.VMEM((8, DH), F32),
            pltpu.VMEM((seq_count, 8, DH), F32),
            pltpu.VMEM((8, DH), F32),
            pltpu.VMEM((dp_count, 8, DH), F32),
            dma((4,)),
            dma((4,)),
            dma((seq_count,)),
            dma((seq_count,)),
            dma((2, moves)),
            dma((2, CHIPS, 2)),
            dma((2, hops)),
            dma((2, 5)),
            dma((4,)),
            dma((4,)),
            dma((2, max(seq_count, dp_count))),
            dma((2, max(seq_count, dp_count))),
        ],
        compiler_params=pltpu.CompilerParams(
            collective_id=0, has_side_effects=True, vmem_limit_bytes=48 * 1024 * 1024
        ),
        name="routed_attention",
    )(queries, key_vectors, values, out_grad, positions, sink_logits)
    return (*outs[:4], outs[4][0, :CORES])


def solution(mesh):
    rows = P("dp", ("seq", "tensor"), None)
    return jax.shard_map(
        on_device,
        mesh=mesh,
        in_specs=(rows, rows, rows, rows, P("dp", "seq"), P("tensor")),
        out_specs=(rows, rows, rows, rows, P("tensor")),
        check_vma=False,
    )
```
